32 devices in a mesh: row: 8 (over z, core), rep: 4 (over y, x).
Axes of the slice: x: 2, y: 2, z: 4, core: 2. Of those that a mesh axis runs over, the one named last changes fastest.
Arguments:
- basis: bfloat16 [32, 65536], P(None, ('row', 'rep')), may hold values from -6 to 6
- precond: float32 [65536], P(('row', 'rep')), may hold values from 0.1 to 0.4
- tiles: bfloat16 [1024, 256, 256], P(('row', 'rep')), as said below
- tile_rows: int32 [1024], P(('row', 'rep')), may hold values from 0 to 31, as said below
- tile_cols: int32 [1024], P(('row', 'rep')), may hold values from 0 to 63, as said below
Outputs:
- directions: float32 [32, 65536], P(None, ('row', 'rep'))
- projected: float32 [64, 64], replicated
The draws below stay inside these ranges and needn't reach their ends.
Inputs may be any that keep to these rules, and one draw needn't show every extreme that they name: The matrix A assembled from all tiles as the steps say is symmetric. `tile_rows`: each device's 32 entries index tile-rows of its band, which are held by the devices of its index along row, in the order of rep. The first 8 entries of a device are its diagonal tiles: the t-th is (index along rep) * 8 + t. Of the other entries none falls in the device's own index along rep, and at most 8 fall in the tile-rows of any one other index along rep, exactly 8 for some. `tile_cols`: each device's 32 entries index tile-columns held by the devices of its index along rep, in the order of row. The first 8 entries of a device are (index along row) * 8 + t for the t-th. Of the other entries none falls in the device's own index along row, and at most 4 fall in the tile-columns of any one other index along row, exactly 4 for some.
All inputs are finite; a program needn't handle non-finite values.
Results may differ from the reference program's by a relative error of at most 0.0003.
Values sent between devices are 32-bit elements; how exact they have to be, the bound alone decides.
No kernel may reach another device: no remote copies, remote signals or barrier semaphores. Data moves between devices by JAX's collectives and lax.ppermute only.
A program may use at most 64 MiB of HBM per device.

```python
import math
import jax
import jax.numpy as jnp
from jax import lax

TB = 256
NEIG = 32
TPD = 8
INNER = 1
PAIRS = 12
TILE_DEV = 32
NN = 65536
N_ROW = 8
N_REP = 4


outer_level = 1.3


inner_level = 1.0


def shift_list(count, slots):
    return 1 + ((slots + 1) * (count // 2) - 1) % (count - 1)


def layout(key):
    devices = N_ROW * N_REP
    sources = jnp.arange(devices, dtype=jnp.int32)
    row_of = sources // N_REP
    rep_of = sources % N_REP
    slots = jnp.arange(PAIRS, dtype=jnp.int32)
    row_shift = shift_list(N_ROW, slots)
    rep_shift = shift_list(N_REP, slots)
    target_row = (row_of[None, :] + row_shift[:, None]) % N_ROW
    target_rep = (rep_of[None, :] + rep_shift[:, None]) % N_REP
    source_row = (row_of[None, :] - row_shift[:, None]) % N_ROW
    source_rep = (rep_of[None, :] - rep_shift[:, None]) % N_REP
    inverse = (source_row * N_REP + source_rep).astype(jnp.int32)
    first_offset = jax.random.randint(jax.random.fold_in(key, 102), (PAIRS, devices), 0, TPD, dtype=jnp.int32)
    second_offset = jax.random.randint(jax.random.fold_in(key, 103), (PAIRS, devices), 0, TPD, dtype=jnp.int32)
    own_rows = target_rep * TPD + first_offset
    own_cols = target_row * TPD + second_offset
    back_rows = source_rep * TPD + jnp.take_along_axis(second_offset, inverse, axis=1)
    back_cols = source_row * TPD + jnp.take_along_axis(first_offset, inverse, axis=1)
    steps_local = jnp.arange(TPD, dtype=jnp.int32)[None, :]
    diagonal_rows = rep_of[:, None] * TPD + steps_local
    diagonal_cols = row_of[:, None] * TPD + steps_local
    all_rows = jnp.concatenate([diagonal_rows, own_rows.T, back_rows.T], axis=1).reshape(-1)
    all_cols = jnp.concatenate([diagonal_cols, own_cols.T, back_cols.T], axis=1).reshape(-1)
    return (all_rows.astype(jnp.int32), all_cols.astype(jnp.int32), inverse)


def draw_tile_rows(key, part):
    return layout(key)[0]


def draw_tile_cols(key, part):
    return layout(key)[1]


def draw_tiles(key, part):
    devices = N_ROW * N_REP
    inverse = layout(key)[2]
    slot_index = jnp.arange(PAIRS, dtype=jnp.int32)[:, None]
    slot_order = jax.random.permutation(jax.random.fold_in(key, 107), jnp.arange(PAIRS, dtype=jnp.int32))
    ladder = 0.5 * jnp.power(4.0, slot_order.astype(jnp.float32) / max(PAIRS - 1, 1))
    outer_tiles = jax.random.normal(jax.random.fold_in(key, 104), (PAIRS, devices, TB, TB), jnp.float32) * (outer_level / jnp.sqrt(1.0 * TB))
    outer_tiles = outer_tiles * ladder[:, None, None, None]
    mirrored = jnp.swapaxes(outer_tiles[slot_index, inverse], 2, 3)
    noise = jax.random.normal(jax.random.fold_in(key, 105), (devices, TPD, TB, TB), jnp.float32) * (inner_level / jnp.sqrt(1.0 * TB))
    levels = jax.random.uniform(jax.random.fold_in(key, 106), (devices, TPD, TB), jnp.float32, 3.0, 5.0)
    identity = jnp.eye(TB, dtype=jnp.float32)
    diagonal_tiles = 0.5 * (noise + jnp.swapaxes(noise, 2, 3)) + levels[:, :, :, None] * identity[None, None, :, :]
    whole = jnp.concatenate([diagonal_tiles, jnp.swapaxes(outer_tiles, 0, 1), jnp.swapaxes(mirrored, 0, 1)], axis=1)
    return whole.reshape(-1, TB, TB).astype(jnp.bfloat16)


def block_levels(key, extent, shards, least, top_value):
    def one(dim, blocks):
        steps = jax.random.uniform(jax.random.fold_in(jax.random.fold_in(key, 6), dim), (blocks,), jnp.float32, least / len(shards), top_value / len(shards))
        return jnp.repeat(jnp.exp(steps), extent[dim] // blocks).reshape((-1,) + (1,) * (len(extent) - dim - 1))

    factor_of = one(*shards[0])
    for cut in shards[1:]:
        factor_of = factor_of * one(*cut)
    return factor_of


def bell_draw(own_key, extent, width, bound, split=(), kind=jnp.bfloat16):
    gain = block_levels(own_key, extent, split, -0.22, 0.18) if split else 1.0
    array = jax.random.normal(own_key, extent, jnp.float32) * width * gain
    return jnp.minimum(jnp.maximum(array, -bound), bound).astype(kind)


def setup_inputs(seed: int = 0) -> dict:
    seeds = jax.random.split(jax.random.key(seed), 6)
    basis = bell_draw(seeds[0], (NEIG, NN), 1.0, 6.0, ((1, 32),))
    precond = jnp.clip(jnp.exp(math.log(0.4) - 1.3862944 * jax.random.uniform(seeds[1], (NN,), jnp.float32) ** block_levels(seeds[1], (NN,), ((0, 32),), -0.2, 0.2)), 0.1, 0.4)
    tiles = draw_tiles(jax.random.fold_in(seeds[5], 71), 0)
    tile_rows = draw_tile_rows(jax.random.fold_in(seeds[5], 71), 0)
    tile_cols = draw_tile_cols(jax.random.fold_in(seeds[5], 71), 0)
    return dict(basis=basis, precond=precond, tiles=tiles, tile_rows=tile_rows, tile_cols=tile_cols)


def apply_matrix(vectors, tiles, tile_rows, tile_cols):
    devices = N_ROW * N_REP
    band = N_REP * TPD * TB
    tiles_grouped = tiles.reshape(devices, TILE_DEV, TB, TB)
    rows_grouped = tile_rows.reshape(devices, TILE_DEV)
    cols_grouped = tile_cols.reshape(devices, TILE_DEV)
    offsets = jnp.arange(TB, dtype=jnp.int32)
    bands = jnp.arange(N_REP * TPD, dtype=jnp.int32)

    def accumulate(total, item):
        tile_block, row_local, col_local, device = item
        band_index = device // N_REP
        column_set = device % N_REP
        global_cols = (col_local // TPD * N_REP + column_set) * TPD + col_local % TPD
        positions = (global_cols[:, None] * TB + offsets[None, :]).reshape(-1).astype(jnp.int32)
        picked = jnp.take(vectors, positions, axis=1).reshape(NEIG, TILE_DEV, TB)
        products = jnp.einsum('kjc,jrc->kjr', picked.astype(jnp.float32), tile_block.astype(jnp.float32), precision=lax.Precision.HIGHEST)
        selector = (row_local[:, None] == bands[None, :]).astype(jnp.float32)
        partial_value = jnp.einsum('kjr,jb->kbr', products, selector, precision=lax.Precision.HIGHEST).reshape(NEIG, band)
        begin = (band_index * band).astype(jnp.int32)
        zero_index = jnp.zeros((), jnp.int32)
        current = lax.dynamic_slice(total, (zero_index, begin), (NEIG, band))
        total = lax.dynamic_update_slice(total, current + partial_value, (zero_index, begin))
        return (total, None)
    start_total = jnp.zeros((NEIG, NN), jnp.float32)
    total, unused = lax.scan(accumulate, start_total, (tiles_grouped, rows_grouped, cols_grouped, jnp.arange(devices, dtype=jnp.int32)))
    return total

def reference(basis, precond, tiles, tile_rows, tile_cols):
    highest = lax.Precision.HIGHEST
    basis_float = basis.astype(jnp.float32)

    def project(block):
        coefficients = jnp.dot(block, basis_float.T, precision=highest) / NN
        return block - jnp.dot(coefficients, basis_float, precision=highest)
    applied = apply_matrix(basis_float, tiles, tile_rows, tile_cols)
    ritz_values = jnp.sum(basis_float * applied, axis=1) / NN
    residual = applied - ritz_values[:, None] * basis_float
    correlation = jnp.dot(residual, basis_float.T, precision=highest) / NN
    right_side = -(residual - jnp.dot(correlation, basis_float, precision=highest))
    correction = project(precond[None, :] * right_side)
    for iteration in range(INNER):
        image_block = apply_matrix(correction, tiles, tile_rows, tile_cols)
        updated = correction + precond[None, :] * (right_side - (image_block - ritz_values[:, None] * correction))
        correction = project(updated)
    correction_gram = jnp.dot(correction, correction.T, precision=highest) / NN
    factor = jnp.linalg.cholesky(correction_gram)
    directions = lax.linalg.triangular_solve(factor, correction, left_side=True, lower=True)
    adirections = apply_matrix(directions, tiles, tile_rows, tile_cols)
    block_basis = jnp.dot(basis_float, applied.T, precision=highest) / NN
    block_cross = jnp.dot(basis_float, adirections.T, precision=highest) / NN
    block_new = jnp.dot(directions, adirections.T, precision=highest) / NN
    upper = jnp.concatenate([block_basis, block_cross], axis=1)
    lower = jnp.concatenate([block_cross.T, block_new], axis=1)
    projected = jnp.concatenate([upper, lower], axis=0)
    return (directions, projected)
```

```python
import functools
import jax
import jax.numpy as jnp
from jax import lax
from jax.experimental import pallas as pl
from jax.experimental.pallas import tpu as pltpu
from jax.sharding import PartitionSpec as P

F32 = jnp.float32
BF16 = jnp.bfloat16
HIGHEST = lax.Precision.HIGHEST
ROW, REP = "row", "rep"


def xor_move(value, axis, mask):
    count = lax.axis_size(axis)
    return lax.ppermute(value, axis, [(i, i ^ mask) for i in range(count)])


def split(value, terms):
    parts = []
    rest = value
    for i in range(terms):
        part = rest.astype(BF16)
        parts.append(part)
        if i + 1 < terms:
            rest = rest - part.astype(F32)
    return parts


def fold(value, rows):
    total = value[:rows]
    for i in range(1, value.shape[0] // rows):
        total = total + value[i * rows : (i + 1) * rows]
    return total


def dot_nt(left, right):
    return lax.dot_general(left, right, (((1,), (1,)), ((), ())), preferred_element_type=F32)


def dot_nn(left, right):
    return lax.dot_general(left, right, (((1,), (0,)), ((), ())), preferred_element_type=F32)


def small_nt(left, right):
    rows = left.shape[0]
    stacked = jnp.concatenate(split(left, 3), axis=0)
    total = None
    for part in split(right, 3):
        one = dot_nt(stacked, part)
        total = one if total is None else total + one
    return fold(total, rows)


def full_dot(left, right):
    return jnp.dot(left, right, precision=HIGHEST, preferred_element_type=F32)


def full_nt(left, right):
    return lax.dot_general(
        left, right, (((1,), (1,)), ((), ())), precision=HIGHEST, preferred_element_type=F32
    )


VMEM = pl.BlockSpec(memory_space=pltpu.VMEM)
SMEM = pl.BlockSpec(memory_space=pltpu.SMEM)


def call(kernel, name, outs, smem, args, scratch=()):
    return pl.pallas_call(
        kernel,
        name=name,
        out_shape=[jax.ShapeDtypeStruct(s, d) for s, d in outs],
        in_specs=[SMEM] * smem + [VMEM] * (len(args) - smem),
        out_specs=[VMEM] * len(outs),
        scratch_shapes=list(scratch),
    )(*args)


def multiply_tiles(index_of, rows_ref, tiles_ref, xs_ref, acc_ref, rep, tiles_each, columns, group=4):
    tile_count = tiles_ref.shape[0]

    def step(g, carry):
        products = []
        for i in range(group):
            j = g * group + i
            slot, weight = index_of(j)
            product = fold(dot_nt(xs_ref[slot], tiles_ref[j]), columns)
            if weight is not None:
                product = product * weight
            products.append(product)
        for i in range(group):
            row = rows_ref[g * group + i]
            place = lax.bitwise_xor(row // tiles_each, rep) * tiles_each + row % tiles_each
            acc_ref[place] = acc_ref[place] + products[i]
        return carry

    lax.fori_loop(0, tile_count // group, step, 0)


def fill_terms(x_refs, xs_ref, tiles_each, columns, terms):
    for m, x_ref in enumerate(x_refs):

        def one(t, carry, m=m, x_ref=x_ref):
            for i, part in enumerate(split(x_ref[t], terms)):
                xs_ref[m * tiles_each + t, i * columns : (i + 1) * columns, :] = part
            return carry

        lax.fori_loop(0, tiles_each, one, 0)


def shards(basis, precond, tiles, tile_rows, tile_cols):
    columns = basis.shape[0]
    shard_rows = basis.shape[1]
    tile_size = tiles.shape[1]
    tiles_each = shard_rows // tile_size
    row_count = lax.axis_size(ROW)
    rep_count = lax.axis_size(REP)
    chips = row_count // 2
    inverse_count = 1.0 / (shard_rows * row_count * rep_count)
    block = (tiles_each, columns, tile_size)
    small = (columns, columns)
    band_slots = rep_count * tiles_each
    place = jnp.stack([lax.axis_index(ROW), lax.axis_index(REP)]).astype(jnp.int32)
    scaling = precond.reshape(tiles_each, 1, tile_size)

    def groups(bits):
        return [bits[i : i + 2] for i in range(0, len(bits), 2)]

    def sum_over(value, axis, bits):
        if len(bits) == 1:
            return value + xor_move(value, axis, bits[0])
        one, two = bits
        near = xor_move(value, axis, one)
        far = xor_move(value, axis, two)
        both = xor_move(value, axis, one | two)
        return (value + near) + (far + both)

    def bits_of(count, first):
        return [1 << i for i in range(first, count.bit_length() - 1)]

    def sum_all(value):
        value = sum_over(value, ROW, [1])
        for bits in groups(bits_of(rep_count, 0)):
            value = sum_over(value, REP, bits)
        for bits in groups(bits_of(row_count, 1)):
            value = sum_over(value, ROW, bits)
        return value

    def gather_row(value):
        same = [value] + [xor_move(value, ROW, 2 * k) for k in range(1, chips)]
        other = [xor_move(v, ROW, 1) for v in same]
        return [v for pair in zip(same, other) for v in pair]

    def gather_rep(value):
        return [value] + [xor_move(value, REP, k) for k in range(1, rep_count)]

    def scatter_rep(parts):
        return [parts[0]] + [xor_move(parts[k], REP, k) for k in range(1, rep_count)]

    pad_rows = 8

    def prepare_kernel(basis_ref, scaling_ref, block_ref, band_ref):
        for t in range(tiles_each):
            value = basis_ref[:, t * tile_size : (t + 1) * tile_size].astype(F32)
            block_ref[t] = value
            band_ref[t, :columns, :] = value
            band_ref[t, columns:, :] = jnp.broadcast_to(scaling_ref[t], (pad_rows, tile_size))

    basis_block, basis_band = call(
        prepare_kernel,
        "prepare",
        [(block, F32), ((tiles_each, columns + pad_rows, tile_size), F32)],
        0,
        (basis, scaling),
    )

    def product_kernel(terms, with_band):
        def kernel(place_ref, rows_ref, cols_ref, tiles_ref, *refs):
            x_refs, refs = refs[:row_count], refs[row_count:]
            if with_band:
                band_refs, refs = refs[:rep_count], refs[rep_count:]
            out_refs, refs = refs[:rep_count], refs[rep_count:]
            if with_band:
                small_ref, refs = refs[0], refs[1:]
            xs_ref, acc_ref = refs
            row, rep = place_ref[0], place_ref[1]
            fill_terms(x_refs, xs_ref, tiles_each, columns, terms)
            acc_ref[...] = jnp.zeros(acc_ref.shape, F32)

            def index_of(j):
                col = cols_ref[j]
                slot = lax.bitwise_xor(col // tiles_each, row) * tiles_each + col % tiles_each
                return slot, None

            multiply_tiles(index_of, rows_ref, tiles_ref, xs_ref, acc_ref, rep, tiles_each, columns)
            for k in range(rep_count):
                out_refs[k][...] = acc_ref[k * tiles_each : (k + 1) * tiles_each]
            if with_band:
                totals = [jnp.zeros((3 * columns, columns), F32)] * 2
                for k in range(rep_count):

                    def one(t, carry, k=k):
                        plain, scaled = carry
                        left = jnp.concatenate(split(acc_ref[k * tiles_each + t], 3), axis=0)
                        rows = band_refs[k][t, :columns, :]
                        plain = plain + dot_nt(left, rows.astype(BF16))
                        weighted = rows * band_refs[k][t, columns : columns + 1, :]
                        for part in split(weighted, 3):
                            scaled = scaled + dot_nt(left, part)
                        return plain, scaled

                    totals = lax.fori_loop(0, tiles_each, one, tuple(totals))
                own = [jnp.zeros((columns, columns), F32), jnp.zeros((3 * columns, columns), F32)]
                for t in range(tiles_each):
                    rows = band_refs[0][t, :columns, :]
                    weighted = rows * band_refs[0][t, columns : columns + 1, :]
                    narrow = rows.astype(BF16)
                    own[0] = own[0] + dot_nt(narrow, narrow)
                    own[1] = own[1] + dot_nt(jnp.concatenate(split(weighted, 3), axis=0), narrow)
                pieces = [fold(totals[0], columns), fold(totals[1], columns), own[0], fold(own[1], columns)]
                small_ref[...] = jnp.concatenate([p * inverse_count for p in pieces], axis=1)

        return kernel

    def products(x_blocks, band, terms):
        with_band = band is not None
        outs = [(block, F32)] * rep_count
        if with_band:
            outs = outs + [((columns, 4 * columns), F32)]
        return call(
            product_kernel(terms, with_band),
            "products_band" if with_band else "products",
            outs,
            3,
            (place, tile_rows, tile_cols, tiles, *x_blocks, *(band or ())),
            [
                pltpu.VMEM((row_count * tiles_each, terms * columns, tile_size), BF16),
                pltpu.VMEM((band_slots, columns, tile_size), F32),
            ],
        )

    row_blocks = gather_row(basis_block)
    band_blocks = gather_rep(basis_band)
    *partial, small_local = products(row_blocks, band_blocks, 1)
    received = scatter_rep(partial)
    basis_small = sum_all(small_local)

    def correct_kernel(small_ref, basis_ref, scaling_ref, *refs):
        parts, (applied_ref, right_ref, correction_ref, ritz_ref) = refs[:rep_count], refs[rep_count:]
        applied_small = small_ref[:, :columns]
        scaled_small = small_ref[:, columns : 2 * columns]
        gram = small_ref[:, 2 * columns : 3 * columns]
        scaled_gram = small_ref[:, 3 * columns : 4 * columns]
        down = lax.broadcasted_iota(jnp.int32, small, 0)
        across = lax.broadcasted_iota(jnp.int32, small, 1)
        diagonal = jnp.where(down == across, applied_small, 0.0)
        ritz = jnp.sum(diagonal, axis=1, keepdims=True)
        correlation = applied_small - ritz * gram
        coefficients = -scaled_small + ritz * scaled_gram + full_dot(correlation, scaled_gram)
        mix = correlation + diagonal
        stacked = jnp.concatenate(split(mix, 3) + split(coefficients, 3), axis=0)
        for t in range(tiles_each):
            total = parts[0][t]
            for part in parts[1:]:
                total = total + part[t]
            applied_ref[t] = total
            mixed = dot_nn(stacked, basis_ref[t].astype(BF16))
            right = fold(mixed[: 3 * columns], columns) - total
            right_ref[t] = right
            correction_ref[t] = scaling_ref[t] * right - fold(mixed[3 * columns :], columns)
        ritz_ref[...] = ritz

    applied, right_side, correction, ritz = call(
        correct_kernel,
        "correct",
        [(block, F32), (block, F32), (block, F32), ((columns, 1), F32)],
        0,
        (basis_small, basis_block, scaling, *received),
    )

    received = scatter_rep(products(gather_row(correction), None, 3))

    def update_kernel(ritz_ref, basis_ref, scaling_ref, applied_ref, right_ref, correction_ref, *refs):
        parts, (updated_ref, small_ref) = refs[:rep_count], refs[rep_count:]
        ritz = ritz_ref[...]
        totals = [jnp.zeros((3 * columns, columns), F32)] * 3
        for t in range(tiles_each):
            image = parts[0][t]
            for part in parts[1:]:
                image = image + part[t]
            start = correction_ref[t]
            updated = start + scaling_ref[t] * (right_ref[t] - (image - ritz * start))
            updated_ref[t] = updated
            terms = split(updated, 3)
            left = jnp.concatenate(terms, axis=0)
            totals[0] = totals[0] + dot_nt(left, basis_ref[t].astype(BF16))
            for term in terms:
                totals[1] = totals[1] + dot_nt(left, term)
            for term in split(applied_ref[t], 3):
                totals[2] = totals[2] + dot_nt(left, term)
        pieces = [fold(total, columns) * inverse_count for total in totals]
        small_ref[...] = jnp.concatenate(pieces + [jnp.zeros(small, F32)], axis=1)

    updated, small_local = call(
        update_kernel,
        "update",
        [(block, F32), ((columns, 4 * columns), F32)],
        0,
        (ritz, basis_block, scaling, applied, right_side, correction, *received),
    )

    half = chips // 2

    def gather_half(value):
        same = [value]
        for d in range(1, half + 1):
            if d < half or chips == 1:
                pairs = [((z + d) % chips, z) for z in range(chips)]
            else:
                pairs = [(z + half, z) if z % 2 else (z, z + half) for z in range(half)]
            moves = [(2 * a + c, 2 * b + c) for a, b in pairs for c in range(2)]
            same.append(lax.ppermute(value, ROW, moves))
        other = [xor_move(v, ROW, 1) for v in same]
        return [v for pair in zip(same, other) for v in pair]

    half_blocks = gather_half(updated)
    updated_band = gather_rep(updated)
    update_small = sum_all(small_local)

    def quadratic_kernel(place_ref, rows_ref, cols_ref, tiles_ref, *refs):
        x_refs, refs = refs[: len(half_blocks)], refs[len(half_blocks) :]
        band_refs, (out_ref, xs_ref, acc_ref) = refs[:rep_count], refs[rep_count:]
        row, rep = place_ref[0], place_ref[1]
        chip, core = row // 2, row % 2
        fill_terms(x_refs, xs_ref, tiles_each, columns, 3)
        acc_ref[...] = jnp.zeros(acc_ref.shape, F32)
        takes_middle = jnp.where(chip < half, chip % 2 == 1, (chip - half) % 2 == 0)

        def index_of(j):
            col = cols_ref[j]
            owner = col // tiles_each
            distance = (owner // 2 - chip + chips) % chips
            used = (distance < half) | ((distance == half) & takes_middle)
            weight = jnp.where(distance == 0, 0.5, jnp.where(used, 1.0, 0.0)).astype(F32)
            peer = jnp.where(used, 2 * distance + lax.bitwise_xor(owner % 2, core), 0)
            return peer * tiles_each + col % tiles_each, weight

        multiply_tiles(index_of, rows_ref, tiles_ref, xs_ref, acc_ref, rep, tiles_each, columns)
        total = jnp.zeros((3 * columns, columns), F32)
        for k in range(rep_count):

            def one(t, carry, k=k):
                left = jnp.concatenate(split(acc_ref[k * tiles_each + t], 3), axis=0)
                for part in split(band_refs[k][t], 3):
                    carry = carry + dot_nt(left, part)
                return carry

            total = lax.fori_loop(0, tiles_each, one, total)
        out_ref[...] = fold(total, columns) * inverse_count

    (quadratic,) = call(
        quadratic_kernel,
        "quadratic",
        [(small, F32)],
        3,
        (place, tile_rows, tile_cols, tiles, *half_blocks, *updated_band),
        [
            pltpu.VMEM((len(half_blocks) * tiles_each, 3 * columns, tile_size), BF16),
            pltpu.VMEM((band_slots, columns, tile_size), F32),
        ],
    )
    quadratic = sum_all(quadratic)

    applied_small = basis_small[:, :columns]
    gram = basis_small[:, 2 * columns : 3 * columns]
    along = update_small[:, :columns]
    cross = full_nt(along, along)
    correction_gram = (
        update_small[:, columns : 2 * columns]
        - cross
        - cross.T
        + full_nt(full_dot(along, gram), along)
    )
    factor = jnp.linalg.cholesky(correction_gram)
    inverse = lax.linalg.triangular_solve(factor, jnp.eye(columns, dtype=F32), left_side=True, lower=True)

    def directions_kernel(inverse_ref, along_ref, updated_ref, basis_ref, out_ref):
        inverse_terms = jnp.concatenate(split(inverse_ref[...], 3), axis=0)
        along_terms = jnp.concatenate(split(along_ref[...], 3), axis=0)
        for t in range(tiles_each):
            value = updated_ref[t] - fold(dot_nn(along_terms, basis_ref[t].astype(BF16)), columns)
            total = None
            for part in split(value, 3):
                one = dot_nn(inverse_terms, part)
                total = one if total is None else total + one
            out_ref[:, t * tile_size : (t + 1) * tile_size] = fold(total, columns)

    (directions,) = call(
        directions_kernel,
        "directions",
        [((columns, shard_rows), F32)],
        0,
        (inverse, along, updated, basis_block),
    )

    def projected_kernel(quadratic_ref, inverse_ref, basis_small_ref, update_small_ref, out_ref):
        inverse_value = inverse_ref[...]
        applied_value = basis_small_ref[:, :columns]
        along_value = update_small_ref[:, :columns]
        mixed = update_small_ref[:, 2 * columns : 3 * columns]
        reduced = mixed - full_nt(along_value, applied_value)
        lower = full_dot(inverse_value, reduced)
        outer = full_nt(along_value, mixed)
        inner = full_nt(full_dot(along_value, applied_value), along_value)
        middle = quadratic_ref[...] + quadratic_ref[...].T - outer - outer.T + inner
        new = full_nt(full_dot(inverse_value, middle), inverse_value)
        out_ref[:columns, :columns] = applied_value.T
        out_ref[:columns, columns:] = lower.T
        out_ref[columns:, :columns] = lower
        out_ref[columns:, columns:] = new

    (projected,) = call(
        projected_kernel,
        "projected",
        [((2 * columns, 2 * columns), F32)],
        0,
        (quadratic, inverse, basis_small, update_small),
    )
    return (directions, projected)


def solution(mesh):
    in_specs = (
        P(None, (ROW, REP)),
        P((ROW, REP)),
        P((ROW, REP), None, None),
        P((ROW, REP)),
        P((ROW, REP)),
    )
    out_specs = (P(None, (ROW, REP)), P())
    return jax.shard_map(shards, mesh=mesh, in_specs=in_specs, out_specs=out_specs, check_vma=False)
```
